32 devices in a mesh: dp: 8 (over z, x), expert: 4 (over y, core).
Axes of the slice: x: 2, y: 2, z: 4, core: 2. Of those that a mesh axis runs over, the one named last changes fastest.
Arguments:
- tokens: bfloat16 [4096, 2048], P(('dp', 'expert')), may hold values from -6 to 6
- cotangent: bfloat16 [4096, 2048], P(('dp', 'expert')), may hold values from -6 to 6
- expert_ids: int32 [4096, 2], P(('dp', 'expert')), may hold values from 0 to 3, all different within a row; in each aligned block of 128 rows (0 to 127, 128 to 255, ...) at most 72 rows name the same one
- route_share: float32 [4096], P(('dp', 'expert')), may hold values from 0.5 to 0.95
- gate_proj: bfloat16 [4, 7168, 2048], P('expert', 'dp'), may hold values from -0.125 to 0.125
- up_proj: bfloat16 [4, 7168, 2048], P('expert', 'dp'), may hold values from -0.125 to 0.125
- down_anchor: float32 [4, 7168, 2048], P('expert', 'dp'), may hold values from -0.12 to 0.12
- down_average: float32 [4, 7168, 2048], P('expert', 'dp'), may hold values from -0.12 to 0.12
- down_moment: float32 [4, 7168, 2048], P('expert', 'dp'), may hold values from 0.002 to 0.05
Outputs:
- new_anchor: float32 [4, 7168, 2048], P('expert', 'dp')
- new_average: float32 [4, 7168, 2048], P('expert', 'dp')
- new_moment: float32 [4, 7168, 2048], P('expert', 'dp')
The draws below stay inside these ranges and needn't reach their ends.
Inputs may be any that keep to these rules, and one draw needn't show every extreme that they name: `expert_ids`: the two ids of a token differ. The rows of one device name any expert at most 72 times, and in every draw some device names some expert exactly 72 times.
All inputs are finite; a program needn't handle non-finite values.
Results may differ from the reference program's by a relative error of at most 0.0043.
Values may be sent and summed in bfloat16 or wider, within the bound.
A program may use at most 192 MiB of HBM per device.

```python
import math
import jax
import jax.numpy as jnp
import numpy as np
from jax import lax

D = 2048
FF = 7168
TOPK = 2
TOK_DEV = 128
EXPERTS = 4
CAP = 72
TOKENS = 4096
DEVICES = 32


def shard_levels(rng, extent, pieces, least, top_value):
    def one(position, blocks):
        draws = jax.random.uniform(jax.random.fold_in(jax.random.fold_in(rng, 6), position), (blocks,), jnp.float32, least / len(pieces), top_value / len(pieces))
        return jnp.repeat(jnp.exp(draws), extent[position] // blocks).reshape((-1,) + (1,) * (len(extent) - position - 1))

    gain = one(*pieces[0])
    for cut in pieces[1:]:
        gain = gain * one(*cut)
    return gain


def routed_block(key, own, number, rows, number_of, top, most, skew):
    order = jax.random.permutation(key, number_of)
    crowded, common = portions_of(number_of, rows * top, most, skew, True), portions_of(number_of, rows * top, most, skew, False)
    places = jnp.arange(number_of)

    def named(sizes, rotation):
        used = int((sizes > 0).sum())
        fixed = max(1, used // 4)
        passed = fixed + (places - fixed + rotation * (used - fixed)) % max(1, number_of - fixed)
        return jnp.zeros((number_of,), jnp.int32).at[order[jnp.where(places < fixed, places, passed)]].set(jnp.asarray(sizes, jnp.int32))

    sizes = jnp.where(number % 4 == 0, named(crowded, number // 4), named(common, number - number // 4 - 1))
    mixed = jax.random.permutation(jax.random.fold_in(own, 3), number_of)
    donor, sink = mixed[0:number_of // 2 * 2:2], mixed[1:number_of // 2 * 2:2]
    margin = jnp.minimum(sizes[donor] - 1, most - sizes[sink]) // 2
    margin = jnp.where((donor == order[0]) | (sink == order[0]) | (sizes[sink] == 0), 0, jnp.maximum(margin, 0))
    passed = jax.random.randint(jax.random.fold_in(own, 4), (number_of // 2,), 0, 1 << 20) % (margin + 1)
    sizes = sizes.at[donor].add(-passed).at[sink].add(passed)
    members = jnp.searchsorted(jnp.cumsum(sizes), jnp.arange(rows * top), side="right").astype(jnp.int32)
    listing = members.reshape(top, rows).T
    listing = listing[jax.random.permutation(jax.random.fold_in(own, 1), rows)]
    rotation = jax.random.randint(jax.random.fold_in(own, 2), (rows, 1), 0, top)
    return jnp.take_along_axis(listing, (jnp.arange(top)[None, :] + rotation) % top, axis=1)


def portions_of(number_of, total, limit, skew, full):
    portions = [(1 << 20) // math.isqrt(rank ** skew) + 1 for rank in range(1, number_of + 1)]
    largest = limit if full else min(limit, max(-(-total // number_of), total * portions[0] // sum(portions)))
    least = 1 if total - largest >= number_of - 1 else 0
    holding, surplus = [largest] + [least] * (number_of - 1), total - largest - least * (number_of - 1)
    while surplus > 0:
        candidates = [i for i in range(1, number_of) if holding[i] < largest] or [i for i in range(1, number_of) if holding[i] < limit]
        pool, left = sum([portions[i] for i in candidates]), surplus
        for i in candidates:
            extra = min(limit - holding[i], max(1, left * portions[i] // pool), surplus)
            holding[i] = holding[i] + extra
            surplus = surplus - extra
    return np.array(holding)


def noise(stream_key, shape, spread, reach, split=(), kind=jnp.bfloat16):
    entries = jax.random.normal(stream_key, shape, jnp.float32) * spread
    if len(split) > 0:
        entries = shard_levels(stream_key, shape, split, -0.22, 0.18) * entries
    return jnp.clip(entries, min=-reach, max=reach).astype(kind)


def setup_inputs(seed: int = 0) -> dict:
    streams_of = jax.random.split(jax.random.key(seed), 10)
    tokens = noise(streams_of[0], (TOKENS, D), 1.0, 6.0, ((0, 32),))
    cotangent = noise(streams_of[1], (TOKENS, D), 1.0, 6.0, ((0, 32),))
    expert_ids_keys = jax.random.split(jax.random.fold_in(streams_of[2], 1), TOKENS // TOK_DEV)
    expert_ids_turns = jax.random.permutation(jax.random.fold_in(streams_of[2], 3), TOKENS // TOK_DEV)
    expert_ids = jax.vmap(lambda own, number: routed_block(jax.random.fold_in(streams_of[2], 2), own, number, TOK_DEV, EXPERTS, TOPK, CAP, 1))(expert_ids_keys, expert_ids_turns).reshape((TOKENS, TOPK))
    route_share = jnp.clip(0.5 + 0.45 * jax.random.uniform(streams_of[3], (TOKENS,), jnp.float32) ** shard_levels(streams_of[3], (TOKENS,), ((0, 32),), -0.2, 0.2), 0.5, 0.95)
    gate_proj = noise(streams_of[4], (EXPERTS, FF, D), D ** -0.5, 0.125, ((0, 4), (1, 8)))
    up_proj = noise(streams_of[5], (EXPERTS, FF, D), D ** -0.5, 0.125, ((0, 4), (1, 8)))
    down_anchor = noise(streams_of[6], (EXPERTS, FF, D), 0.02, 0.12, ((0, 4), (1, 8)), jnp.float32)
    down_average = noise(streams_of[7], (EXPERTS, FF, D), 0.02, 0.12, ((0, 4), (1, 8)), jnp.float32)
    down_moment = jnp.clip(jnp.exp(math.log(0.05) - 3.218876 * jax.random.uniform(streams_of[8], (EXPERTS, FF, D), jnp.float32) ** shard_levels(streams_of[8], (EXPERTS, FF, D), ((0, 4), (1, 8)), -0.2, 0.2)), 0.002, 0.05)
    return {"tokens": tokens, "cotangent": cotangent, "expert_ids": expert_ids, "route_share": route_share, "gate_proj": gate_proj, "up_proj": up_proj, "down_anchor": down_anchor, "down_average": down_average, "down_moment": down_moment}


beta_one = 0.9
beta_two = 0.95
learn_rate = 0.05
decay_rate = 0.1
step_count = 4.0
epsilon = 1e-08

def reference(tokens, cotangent, expert_ids, route_share, gate_proj, up_proj, down_anchor, down_average, down_moment):
    shares = jnp.stack([route_share, 1.0 - route_share], axis=1)
    flat_ids = expert_ids.reshape(-1).astype(jnp.int32)
    flat_tok = (jnp.arange(TOKENS * TOPK, dtype=jnp.int32) // TOPK).astype(jnp.int32)
    flat_share = shares.reshape(-1)
    by_expert = jnp.argsort(flat_ids, stable=True).astype(jnp.int32)
    sorted_tok = flat_tok[by_expert]
    gated = (flat_share[by_expert][:, None] * cotangent[sorted_tok].astype(jnp.float32)).astype(jnp.bfloat16)
    rows_in = tokens[sorted_tok]
    expert_range = jnp.arange(EXPERTS, dtype=jnp.int32)
    counts = lax.optimization_barrier(jnp.sum((flat_ids[:, None] == expert_range[None, :]).astype(jnp.int32), axis=0)).astype(jnp.int32)
    starts = (jnp.cumsum(counts) - counts).astype(jnp.int32)
    window = DEVICES * CAP
    pad_rows = jnp.zeros((window, D), jnp.bfloat16)
    rows_in = jnp.concatenate([rows_in, pad_rows], 0)
    gated = jnp.concatenate([gated, pad_rows], 0)

    def one_expert(expert_number):
        begin_row = starts[expert_number]
        xrows = lax.dynamic_slice_in_dim(rows_in, begin_row, window, 0)
        drows = lax.dynamic_slice_in_dim(gated, begin_row, window, 0)
        live_rows = jnp.arange(window, dtype=jnp.int32) < counts[expert_number]
        drows = jnp.where(live_rows[:, None], drows, jnp.zeros_like(drows))
        gate_rows = lax.dynamic_index_in_dim(gate_proj, expert_number, 0, keepdims=False)
        up_rows = lax.dynamic_index_in_dim(up_proj, expert_number, 0, keepdims=False)
        gate_act = jnp.dot(xrows, gate_rows.T, preferred_element_type=jnp.float32)
        up_act = jnp.dot(xrows, up_rows.T, preferred_element_type=jnp.float32)
        hidden = (jax.nn.silu(gate_act) * up_act).astype(jnp.bfloat16)
        return jnp.dot(hidden.T, drows, preferred_element_type=jnp.float32)
    gradient = lax.map(one_expert, expert_range) * FF ** (-0.5)
    bias_two = 1.0 - beta_two ** step_count
    eval_point = (1.0 - beta_one) * down_anchor + beta_one * down_average
    second_moment = beta_two * down_moment + (1.0 - beta_two) * gradient * gradient
    update_dir = gradient / (jnp.sqrt(second_moment / bias_two) + epsilon) + decay_rate * eval_point
    new_anchor = down_anchor - learn_rate * update_dir
    new_average = (1.0 - 1.0 / step_count) * down_average + 1.0 / step_count * new_anchor
    return (new_anchor, new_average, second_moment)
```

```python
import jax
import jax.numpy as jnp
from jax import lax
from jax.sharding import PartitionSpec as P

FF = 7168
TOPK = 2


beta_one = 0.9
beta_two = 0.95
learn_rate = 0.05
decay_rate = 0.1
step_count = 4.0
epsilon = 1e-08


def expert_terms(pieces, weight_gate, weight_up):
    rows_in, gated_rows = pieces
    gate_act = lax.dot_general(
        rows_in, weight_gate, (((1,), (1,)), ((), ())), preferred_element_type=jnp.float32
    )
    up_act = lax.dot_general(
        rows_in, weight_up, (((1,), (1,)), ((), ())), preferred_element_type=jnp.float32
    )
    hidden = (jax.nn.silu(gate_act) * up_act).astype(jnp.bfloat16)
    return lax.dot_general(
        hidden, gated_rows, (((0,), (0,)), ((), ())), preferred_element_type=jnp.float32
    )


def routed_shards(
    tokens,
    cotangent,
    expert_ids,
    route_share,
    gate_proj,
    up_proj,
    down_anchor,
    down_average,
    down_moment,
):
    experts_all = lax.axis_size("expert")
    tok_rows = tokens.shape[0]
    width = tokens.shape[1]
    capacity = tok_rows * TOPK // experts_all * 9 // 8
    slots = experts_all * capacity
    shares = jnp.stack([route_share, 1.0 - route_share], axis=1)
    expert_range = jnp.arange(experts_all, dtype=jnp.int32)
    flat_ids = expert_ids.reshape(-1)
    onehot_routes = (flat_ids[:, None] == expert_range[None, :]).astype(jnp.int32)
    earlier = jnp.cumsum(onehot_routes, axis=0) - onehot_routes
    slot_of = jnp.sum(earlier * onehot_routes, axis=1)
    target = (flat_ids * capacity + slot_of).reshape(tok_rows, TOPK)
    slot_range = jnp.arange(slots, dtype=jnp.int32)
    placed = target[None, :, :] == slot_range[:, None, None]
    picker = jnp.sum(placed.astype(jnp.float32), axis=2).astype(jnp.bfloat16)
    slot_share = jnp.sum(jnp.where(placed, shares[None, :, :], 0.0), axis=(1, 2))
    send_rows = jnp.dot(picker, tokens, preferred_element_type=jnp.float32).astype(jnp.bfloat16)
    send_grad = (
        slot_share[:, None] * jnp.dot(picker, cotangent, preferred_element_type=jnp.float32)
    ).astype(jnp.bfloat16)
    weight_gate = gate_proj[0]
    weight_up = up_proj[0]
    arrived = (
        lax.all_to_all(
            send_rows.reshape(experts_all, capacity, width),
            "expert",
            split_axis=0,
            concat_axis=0,
            tiled=True,
        ),
        lax.all_to_all(
            send_grad.reshape(experts_all, capacity, width),
            "expert",
            split_axis=0,
            concat_axis=0,
            tiled=True,
        ),
    )
    rows_here = arrived[0].reshape(slots, width)
    grad_here = arrived[1].reshape(slots, width)
    gradient = expert_terms(
        (
            lax.all_gather(rows_here, "dp", axis=0, tiled=True),
            lax.all_gather(grad_here, "dp", axis=0, tiled=True),
        ),
        weight_gate,
        weight_up,
    )
    gradient = gradient[None] * FF ** (-0.5)
    bias_two = 1.0 - beta_two**step_count
    eval_point = (1.0 - beta_one) * down_anchor + beta_one * down_average
    second_moment = beta_two * down_moment + (1.0 - beta_two) * gradient * gradient
    update_dir = gradient / (jnp.sqrt(second_moment / bias_two) + epsilon) + decay_rate * eval_point
    new_anchor = down_anchor - learn_rate * update_dir
    new_average = (1.0 - 1.0 / step_count) * down_average + 1.0 / step_count * new_anchor
    return (new_anchor, new_average, second_moment)


def adam(gradient, down_anchor, down_average, down_moment):
    bias_two = 1.0 - beta_two**step_count
    eval_point = (1.0 - beta_one) * down_anchor + beta_one * down_average
    second_moment = beta_two * down_moment + (1.0 - beta_two) * gradient * gradient
    update_dir = gradient / (jnp.sqrt(second_moment / bias_two) + epsilon) + decay_rate * eval_point
    new_anchor = down_anchor - learn_rate * update_dir
    new_average = (1.0 - 1.0 / step_count) * down_average + 1.0 / step_count * new_anchor
    return (new_anchor, new_average, second_moment)


def expert_shares(expert_ids, route_share, experts):
    shares = jnp.stack([route_share, 1.0 - route_share], axis=0)
    expert_range = jnp.arange(experts, dtype=jnp.int32)
    named = expert_ids.T[:, None, :] == expert_range[None, :, None]
    return jnp.sum(jnp.where(named, shares[:, None, :], 0.0), axis=0)


def dense_shards(
    tokens,
    cotangent,
    expert_ids,
    route_share,
    gate_proj,
    up_proj,
    down_anchor,
    down_average,
    down_moment,
):
    experts_all = lax.axis_size("expert")
    axes = ("dp", "expert")
    table = expert_shares(expert_ids, route_share, experts_all)
    share = lax.all_gather(table, axes, axis=1, tiled=True)
    share = lax.dynamic_index_in_dim(share, lax.axis_index("expert"), 0, keepdims=True)
    rows = lax.all_gather(tokens, axes, axis=0, tiled=True)
    grads = lax.all_gather(cotangent, axes, axis=0, tiled=True)
    dims = (((1,), (1,)), ((), ()))
    gate_act = lax.dot_general(gate_proj[0], rows, dims, preferred_element_type=jnp.float32)
    up_act = lax.dot_general(up_proj[0], rows, dims, preferred_element_type=jnp.float32)
    hidden = (jax.nn.silu(gate_act) * up_act * share).astype(jnp.bfloat16)
    gradient = jnp.dot(hidden, grads, preferred_element_type=jnp.float32)
    return adam(gradient[None] * FF ** (-0.5), down_anchor, down_average, down_moment)


def solution(mesh):
    placed = (
        P(("dp", "expert"), None),
        P(("dp", "expert"), None),
        P(("dp", "expert"), None),
        P(("dp", "expert")),
        P("expert", "dp", None),
        P("expert", "dp", None),
        P("expert", "dp", None),
        P("expert", "dp", None),
        P("expert", "dp", None),
    )
    shards = dense_shards if mesh.shape["expert"] <= 2 * TOPK else routed_shards
    return jax.shard_map(
        shards,
        mesh=mesh,
        in_specs=placed,
        out_specs=(P("expert", "dp", None), P("expert", "dp", None), P("expert", "dp", None)),
        check_vma=False,
    )
```

```python
import jax
import jax.numpy as jnp
from jax import lax
from jax.experimental import pallas as pl
from jax.experimental.pallas import tpu as pltpu
from jax.sharding import PartitionSpec as P

FF = 7168
TOPK = 2


beta_one = 0.9
beta_two = 0.95
learn_rate = 0.05
decay_rate = 0.1
step_count = 4.0
epsilon = 1e-08


def expert_terms(pieces, weight_gate, weight_up):
    rows_in, gated_rows = pieces
    gate_act = lax.dot_general(
        rows_in, weight_gate, (((1,), (1,)), ((), ())), preferred_element_type=jnp.float32
    )
    up_act = lax.dot_general(
        rows_in, weight_up, (((1,), (1,)), ((), ())), preferred_element_type=jnp.float32
    )
    hidden = (jax.nn.silu(gate_act) * up_act).astype(jnp.bfloat16)
    return lax.dot_general(
        hidden, gated_rows, (((0,), (0,)), ((), ())), preferred_element_type=jnp.float32
    )


def routed_shards(
    tokens,
    cotangent,
    expert_ids,
    route_share,
    gate_proj,
    up_proj,
    down_anchor,
    down_average,
    down_moment,
):
    experts_all = lax.axis_size("expert")
    tok_rows = tokens.shape[0]
    width = tokens.shape[1]
    capacity = tok_rows * TOPK // experts_all * 9 // 8
    slots = experts_all * capacity
    shares = jnp.stack([route_share, 1.0 - route_share], axis=1)
    expert_range = jnp.arange(experts_all, dtype=jnp.int32)
    flat_ids = expert_ids.reshape(-1)
    onehot_routes = (flat_ids[:, None] == expert_range[None, :]).astype(jnp.int32)
    earlier = jnp.cumsum(onehot_routes, axis=0) - onehot_routes
    slot_of = jnp.sum(earlier * onehot_routes, axis=1)
    target = (flat_ids * capacity + slot_of).reshape(tok_rows, TOPK)
    slot_range = jnp.arange(slots, dtype=jnp.int32)
    placed = target[None, :, :] == slot_range[:, None, None]
    picker = jnp.sum(placed.astype(jnp.float32), axis=2).astype(jnp.bfloat16)
    slot_share = jnp.sum(jnp.where(placed, shares[None, :, :], 0.0), axis=(1, 2))
    send_rows = jnp.dot(picker, tokens, preferred_element_type=jnp.float32).astype(jnp.bfloat16)
    send_grad = (
        slot_share[:, None] * jnp.dot(picker, cotangent, preferred_element_type=jnp.float32)
    ).astype(jnp.bfloat16)
    weight_gate = gate_proj[0]
    weight_up = up_proj[0]
    arrived = (
        lax.all_to_all(
            send_rows.reshape(experts_all, capacity, width),
            "expert",
            split_axis=0,
            concat_axis=0,
            tiled=True,
        ),
        lax.all_to_all(
            send_grad.reshape(experts_all, capacity, width),
            "expert",
            split_axis=0,
            concat_axis=0,
            tiled=True,
        ),
    )
    rows_here = arrived[0].reshape(slots, width)
    grad_here = arrived[1].reshape(slots, width)
    gradient = expert_terms(
        (
            lax.all_gather(rows_here, "dp", axis=0, tiled=True),
            lax.all_gather(grad_here, "dp", axis=0, tiled=True),
        ),
        weight_gate,
        weight_up,
    )
    gradient = gradient[None] * FF ** (-0.5)
    bias_two = 1.0 - beta_two**step_count
    eval_point = (1.0 - beta_one) * down_anchor + beta_one * down_average
    second_moment = beta_two * down_moment + (1.0 - beta_two) * gradient * gradient
    update_dir = gradient / (jnp.sqrt(second_moment / bias_two) + epsilon) + decay_rate * eval_point
    new_anchor = down_anchor - learn_rate * update_dir
    new_average = (1.0 - 1.0 / step_count) * down_average + 1.0 / step_count * new_anchor
    return (new_anchor, new_average, second_moment)


def adam(gradient, down_anchor, down_average, down_moment):
    bias_two = 1.0 - beta_two**step_count
    eval_point = (1.0 - beta_one) * down_anchor + beta_one * down_average
    second_moment = beta_two * down_moment + (1.0 - beta_two) * gradient * gradient
    update_dir = gradient / (jnp.sqrt(second_moment / bias_two) + epsilon) + decay_rate * eval_point
    new_anchor = down_anchor - learn_rate * update_dir
    new_average = (1.0 - 1.0 / step_count) * down_average + 1.0 / step_count * new_anchor
    return (new_anchor, new_average, second_moment)


def expert_shares(expert_ids, route_share, experts):
    shares = jnp.stack([route_share, 1.0 - route_share], axis=0)
    expert_range = jnp.arange(experts, dtype=jnp.int32)
    named = expert_ids.T[:, None, :] == expert_range[None, :, None]
    return jnp.sum(jnp.where(named, shares[:, None, :], 0.0), axis=0)


def gather_kernel(
    tok_ref, cot_ref, share_ref, gate_ref, up_ref, acc_ref,
    tok_buf, cot_buf, share_buf, gate_buf, up_buf,
    local_sem, recv_sem, send_sem,
):
    rows = tok_ref.shape[0]
    lanes_of = share_ref.shape[0]
    dp, ex = lax.axis_index("dp"), lax.axis_index("expert")
    layers = lax.axis_size("dp") // 2
    z, x = dp // 2, dp % 2
    y, core = ex // 2, ex % 2
    lower = z < layers // 2
    mirror = lambda v: jnp.where(lower, v, layers - 1 - v)
    depth = mirror(z)
    mid, end = depth == 1, depth == 0
    inner = (jnp.where(lower, z + 1, z - 1) * 2 + x, ex)
    outer = (jnp.where(lower, z - 1, z + 1) * 2 + x, ex)
    over_x = (z * 2 + 1 - x, ex)
    over_y = (dp, (1 - y) * 2 + core)
    partner = (dp, y * 2 + 1 - core)
    layer = (z, mirror(1 - depth), mirror(2), mirror(3))
    OWN, X, Y, D = range(4)
    T, C, S = range(3)

    def chip_of(p, j):
        return (layer[p] * 2 + (x + j % 2) % 2) * 2 + (y + j // 2) % 2

    def slot_of(p, j, c):
        return chip_of(p, j) * 2 + c

    def place(kind, slot):
        if kind == S:
            return share_buf.at[pl.ds(pl.multiple_of(slot * lanes_of, lanes_of), lanes_of), :]
        return (tok_buf, cot_buf)[kind].at[pl.ds(pl.multiple_of(slot * rows, rows), rows), :]

    count = [0]
    always, when_mid = [], []

    def piece(kind, p, j, target, into):
        slot = slot_of(p, j, core)
        copy = pltpu.make_async_remote_copy(
            src_ref=place(kind, slot), dst_ref=place(kind, slot),
            send_sem=send_sem.at[count[0]], recv_sem=recv_sem.at[kind, slot],
            device_id=target, device_id_type=pl.DeviceIdType.MESH,
        )
        count[0] += 1
        into.append(copy)
        return copy

    def send(kinds, p, j, *targets):
        for kind in kinds:
            for target in targets:
                piece(kind, p, j, target, always).start()

    def send_mid(kinds, p, j, target):
        copies = [piece(kind, p, j, target, when_mid) for kind in kinds]

        @pl.when(mid)
        def _():
            for copy in copies:
                copy.start()

    def landed(kind, slot):
        pltpu.make_async_remote_copy(
            src_ref=place(kind, slot), dst_ref=place(kind, slot),
            send_sem=send_sem.at[0], recv_sem=recv_sem.at[kind, slot],
            device_id=partner, device_id_type=pl.DeviceIdType.MESH,
        ).wait_recv()

    def arrive(kinds, p, j):
        for kind in kinds:
            landed(kind, slot_of(p, j, core))
            send((kind,), p, j, partner)

    def arrive_if(cond, kinds, p, j, copies, then=()):
        @pl.when(cond)
        def _():
            for kind, copy in zip(kinds, copies):
                landed(kind, slot_of(p, j, core))
                copy.start()
            for copy in then:
                copy.start()

    def to_partner(kinds, p, j):
        return [piece(kind, p, j, partner, always) for kind in kinds]

    def to_outer(kinds, p, j):
        return [piece(kind, p, j, outer, when_mid) for kind in kinds]

    def unit(chip):
        width = 2 * rows
        at = pl.ds(pl.multiple_of(chip * width, width), width)
        share = jnp.concatenate(
            [share_buf[pl.ds((chip * 2 + c) * lanes_of + ex, 1), :] for c in range(2)], axis=1
        )
        tile = acc_ref.shape[0] // 2
        dims = (((1,), (1,)), ((), ()))

        @pl.loop(0, 2)
        def _(half):
            own = pl.ds(pl.multiple_of(half * tile, tile), tile)
            gate = lax.dot_general(
                gate_buf[own, :], tok_buf[at, :], dims, preferred_element_type=jnp.float32
            )
            up = lax.dot_general(
                up_buf[own, :], tok_buf[at, :], dims, preferred_element_type=jnp.float32
            )
            hidden = (gate / (1.0 + jnp.exp(-gate)) * up * share).astype(jnp.bfloat16)
            acc_ref[own, :] += jnp.dot(hidden, cot_buf[at, :], preferred_element_type=jnp.float32)

    def compute(*units):
        for p, j in units:
            for kind in (T, S, C):
                landed(kind, slot_of(p, j, 1 - core))
        first, number = units[0], len(units)
        if len({p for p, _ in units}) == 1:
            base = layer[first[0]] * 4

            @pl.loop(first[1], first[1] + number)
            def _(j):
                unit(base + (x + j % 2) % 2 * 2 + (y + j // 2) % 2)
        else:
            chips = [chip_of(p, j) for p, j in units]

            @pl.loop(0, number)
            def _(k):
                unit(jnp.where(k == 0, chips[0], chips[1]))

    local = [
        pltpu.make_async_copy(src, dst, local_sem.at[k])
        for k, (src, dst) in enumerate(
            (
                (tok_ref, place(T, slot_of(0, OWN, core))),
                (share_ref, place(S, slot_of(0, OWN, core))),
                (cot_ref, place(C, slot_of(0, OWN, core))),
                (gate_ref, gate_buf),
                (up_ref, up_buf),
            )
        )
    ]
    for copy in local:
        copy.start()
    barrier = pltpu.get_barrier_semaphore()
    for target in (over_x, over_y, partner, inner):
        pl.semaphore_signal(barrier, inc=1, device_id=target, device_id_type=pl.DeviceIdType.MESH)

    @pl.when(mid)
    def _():
        pl.semaphore_signal(barrier, inc=1, device_id=outer, device_id_type=pl.DeviceIdType.MESH)
        pl.semaphore_wait(barrier, 5)

    @pl.when(end)
    def _():
        pl.semaphore_wait(barrier, 4)

    for copy in local[:3]:
        copy.wait()

    TS, CC = (T, S), (C,)
    for kinds in (TS, CC):
        send(kinds, 0, OWN, over_x, over_y, inner)
        send_mid(kinds, 0, OWN, outer)
        send(kinds, 0, OWN, partner)
    for copy in local[3:]:
        copy.wait()

    @pl.loop(0, acc_ref.shape[0] // 64)
    def _(k):
        acc_ref[pl.ds(pl.multiple_of(k * 64, 64), 64), :] = jnp.zeros((64, acc_ref.shape[1]), jnp.float32)

    second = {kinds: (to_partner(kinds, 2, OWN), to_outer(kinds, 2, OWN)) for kinds in (TS, CC)}
    third = {kinds: (to_partner(kinds, 3, OWN), to_outer(kinds, 3, OWN)) for kinds in (TS, CC)}
    across = {kinds: (to_partner(kinds, 2, D), to_outer(kinds, 2, D)) for kinds in (TS, CC)}

    arrive(TS, 0, X)
    send(TS, 0, X, over_y)
    arrive(TS, 0, Y)
    arrive(TS, 1, OWN)
    send_mid(TS, 1, OWN, inner)
    arrive_if(mid, TS, 2, OWN, *second[TS])
    arrive(CC, 0, Y)
    send(CC, 0, Y, over_x)
    arrive(CC, 0, X)
    arrive(CC, 1, OWN)
    send_mid(CC, 1, OWN, inner)
    arrive_if(mid, CC, 2, OWN, *second[CC])
    send(TS + CC, 1, OWN, over_x, over_y)
    arrive(TS + CC, 0, D)
    send(TS + CC, 0, D, inner)
    send_mid(TS + CC, 0, D, outer)
    compute((0, OWN), (0, X), (0, Y), (0, D))

    for kinds in (TS, CC):
        arrive_if(end, kinds, 2, OWN, second[kinds][0])
        send(kinds, 2, OWN, over_x, over_y)
    for kinds in (TS, CC):
        arrive_if(mid, kinds, 3, OWN, *third[kinds])
    for kinds in (TS, CC):
        arrive(kinds, 1, X)
        arrive(kinds, 1, Y)
    compute((1, OWN), (1, X), (1, Y))

    for kinds in (TS, CC):
        arrive(kinds, 2, X)
        arrive(kinds, 2, Y)
    arrive_if(end, TS, 3, OWN, third[TS][0])
    send(TS, 3, OWN, over_x, over_y)
    for kinds in (TS, CC):
        arrive_if(mid, kinds, 2, D, *across[kinds])
    compute((2, OWN), (2, X), (2, Y))

    arrive_if(end, CC, 3, OWN, third[CC][0])
    send(CC, 3, OWN, over_x, over_y)
    arrive(TS + CC, 1, D)
    arrive(TS, 3, X)
    send(TS, 3, X, over_y)
    compute((1, D))
    arrive(TS, 3, Y)
    arrive(CC, 3, Y)
    send(CC, 3, Y, over_x)
    arrive(CC, 3, X)
    compute((3, OWN), (3, X), (3, Y))

    for kinds in (TS, CC):
        arrive_if(end, kinds, 2, D, across[kinds][0])
    arrive(TS + CC, 3, D)
    compute((2, D), (3, D))

    for copy in always:
        copy.wait_send()

    @pl.when(mid)
    def _():
        for copy in when_mid:
            copy.wait_send()


def relay_shards(
    tokens,
    cotangent,
    expert_ids,
    route_share,
    gate_proj,
    up_proj,
    down_anchor,
    down_average,
    down_moment,
):
    experts_all = lax.axis_size("expert")
    devices = experts_all * lax.axis_size("dp")
    rows, width = tokens.shape
    hidden_units = gate_proj.shape[1]
    lines = -(-experts_all // 8) * 8
    table = expert_shares(expert_ids, route_share, lines)
    gradient = pl.pallas_call(
        gather_kernel,
        out_shape=jax.ShapeDtypeStruct((hidden_units, width), jnp.float32),
        in_specs=[pl.BlockSpec(memory_space=pl.ANY)] * 5,
        out_specs=pl.BlockSpec(memory_space=pltpu.VMEM),
        scratch_shapes=[
            pltpu.VMEM((devices * rows, width), jnp.bfloat16),
            pltpu.VMEM((devices * rows, width), jnp.bfloat16),
            pltpu.VMEM((devices * lines, rows), jnp.float32),
            pltpu.VMEM((hidden_units, width), jnp.bfloat16),
            pltpu.VMEM((hidden_units, width), jnp.bfloat16),
            pltpu.SemaphoreType.DMA((5,)),
            pltpu.SemaphoreType.DMA((3, devices)),
            pltpu.SemaphoreType.DMA((192,)),
        ],
        compiler_params=pltpu.CompilerParams(
            collective_id=0, has_side_effects=True, vmem_limit_bytes=62 * 1024 * 1024
        ),
    )(tokens, cotangent, table, gate_proj[0], up_proj[0])
    return adam(gradient[None] * FF ** (-0.5), down_anchor, down_average, down_moment)


def solution(mesh):
    placed = (
        P(("dp", "expert"), None),
        P(("dp", "expert"), None),
        P(("dp", "expert"), None),
        P(("dp", "expert")),
        P("expert", "dp", None),
        P("expert", "dp", None),
        P("expert", "dp", None),
        P("expert", "dp", None),
        P("expert", "dp", None),
    )
    small = (mesh.shape["dp"], mesh.shape["expert"]) == (8, 4)
    shards = relay_shards if small else routed_shards
    return jax.shard_map(
        shards,
        mesh=mesh,
        in_specs=placed,
        out_specs=(P("expert", "dp", None), P("expert", "dp", None), P("expert", "dp", None)),
        check_vma=False,
    )
```
